256 devices in a mesh: tile: 128 (over x, y_lo, z, core), trc: 2 (over y_hi).
Axes of the slice: x: 4, y: 4 (y_hi: 2, y_lo: 2; y = y_hi * 2 + y_lo), z: 8, core: 2. Of those that a mesh axis runs over, the one named last changes fastest.
Arguments:
- tracers: float32 [32, 47, 768, 256], P('trc', None, 'tile'), may hold values from -6 to 6
- courant: float32 [47, 768, 256], P(None, 'tile'), may hold values from -0.4 to 0.4
- vertical_mix: float32 [47, 768, 256], P(None, 'tile'), may hold values from 0.02 to 0.12
- kernel_profile: float32 [47], replicated, may hold values from 0.25 to 1.75
- obs_cell: int32 [262144], P('tile'), may hold values from 0 to 1535
- obs_top: int32 [262144], P('tile'), may hold values from 1 to 47
- obs_count: int32 [128], P('tile'), may hold values from 1 to 2048, 131072 in all
- innovation: float32 [262144], P('tile'), may hold values from -6 to 6
- obs_error: float32 [262144], P('tile'), may hold values from 0.3 to 3
- prior_precision: float32 [32], replicated, may hold values from 0.5 to 2
Outputs:
- fields: float32 [32, 47, 768, 256], P('trc', None, 'tile')
- update: float32 [32], replicated
- misfit: float32 [262144], P('tile')
The draws below stay inside these ranges and needn't reach their ends.
Inputs may be any that keep to these rules, and one draw needn't show every extreme that they name: obs_cell counts cells of the observation's own tile. `obs_count`: the counts sum to 131072 and some tile is full.
All inputs are finite; a program needn't handle non-finite values. No bound on the sum of `obs_count` on one device may be relied on, other than what follows from the above.
Results may differ from the reference program's by a relative error of at most 0.0003.
Values sent between devices are 32-bit elements; how exact they have to be, the bound alone decides.
No kernel may reach another device: no remote copies, remote signals or barrier semaphores. Data moves between devices by JAX's collectives and lax.ppermute only.
A program may use at most 192 MiB of HBM per device.

```python
import math
import jax
import jax.numpy as jnp
import numpy as np
from jax import lax

TRACERS = 32
LEV = 47
LAT = 256
CLON = 6
OBS_CAP = 2048
STEPS = 3
NLON = 768
OBS = 262144
N_TILE = 128


def set_ends(array, stream_key, low, high):
    longest = array.shape.index(max(array.shape))
    spots = []
    for shift in (0, 1):
        where = [jax.random.randint(jax.random.fold_in(stream_key, axis), (), 0, length) for axis, length in enumerate(array.shape)]
        where[longest] = (where[longest] + shift) % array.shape[longest]
        spots.append(tuple(where))
    return array.at[spots[0]].set(low).at[spots[1]].set(high)


def block_scale(key, extent, cuts, low, largest):
    def one(axis_at, shards_of):
        heights = jax.random.uniform(jax.random.fold_in(jax.random.fold_in(key, 6), axis_at), (shards_of,), jnp.float32, low / len(cuts), largest / len(cuts))
        return jnp.repeat(jnp.exp(heights), extent[axis_at] // shards_of).reshape((-1,) + (1,) * (len(extent) - axis_at - 1))

    level = one(*cuts[0])
    for cut in cuts[1:]:
        level = level * one(*cut)
    return level


def profile(number_of, total, most, skew):
    weights = [(1 << 20) // math.isqrt(grade ** skew) + 1 for grade in range(2, number_of + 1)]
    surplus, holding = total - most - (number_of - 1), [1] * (number_of - 1)
    while surplus > 0:
        candidates = [i for i in range(number_of - 1) if holding[i] < most]
        pool, left = sum([weights[i] for i in candidates]), surplus
        for i in candidates:
            addition = min(most - holding[i], max(1, left * weights[i] // pool), surplus)
            holding[i] = holding[i] + addition
            surplus = surplus - addition
    return np.array([most] + holding)


def uneven_parts(stream_key, number_of, total, limit, slope):
    if number_of == 2:
        one = jax.random.randint(stream_key, (), max(1, total - limit), min(limit, total - 1) + 1)
        return jnp.stack([one, total - one])
    tallies = jnp.asarray(profile(number_of, total, limit, slope), jnp.int32)
    couples = (number_of - 1) // 2
    donor, taker = tallies[1:1 + 2 * couples:2], tallies[2:2 + 2 * couples:2]
    margin = jnp.minimum(donor - 1, limit - taker)
    passed = jax.random.randint(jax.random.fold_in(stream_key, 1), (couples,), 0, 1 << 20) % (margin + 1)
    tallies = tallies.at[1:1 + 2 * couples:2].set(donor - passed).at[2:2 + 2 * couples:2].set(taker + passed)
    return tallies[jax.random.permutation(jax.random.fold_in(stream_key, 2), number_of)]


def bell_draw(rng, dims, scale, most, pieces=(), kind=jnp.bfloat16):
    drawn = scale * jax.random.normal(rng, dims, jnp.float32)
    if pieces:
        drawn = drawn * block_scale(rng, dims, pieces, -0.22, 0.18)
    return jnp.clip(drawn, -most, most).astype(kind)


def setup_inputs(seed: int = 0) -> dict:
    splits = jax.random.split(jax.random.key(seed), 11)
    tracers = bell_draw(splits[0], (TRACERS, LEV, NLON, LAT), 1.0, 6.0, ((0, 2), (2, 128)), jnp.float32)
    courant = jnp.clip(jax.random.uniform(splits[1], (LEV, NLON, LAT), jnp.float32, -0.4, 0.4) * block_scale(splits[1], (LEV, NLON, LAT), ((1, 128),), -0.4, 0.0), -0.4, 0.4)
    vertical_mix = jnp.clip(0.02 + 0.09999999776482582 * jax.random.uniform(splits[2], (LEV, NLON, LAT), jnp.float32) ** block_scale(splits[2], (LEV, NLON, LAT), ((1, 128),), -0.2, 0.2), 0.02, 0.12)
    kernel_profile = jnp.clip(1.0 + 0.15 * jax.random.normal(splits[3], (LEV,), jnp.float32), 0.25, 1.75)
    obs_cell = set_ends(jax.random.randint(splits[4], (OBS,), 0, CLON * LAT), jax.random.fold_in(splits[4], 1), 0, (CLON * LAT) - 1).astype(jnp.int32)
    obs_top = set_ends(jax.random.randint(splits[5], (OBS,), 1, LEV + 1), jax.random.fold_in(splits[5], 1), 1, LEV).astype(jnp.int32)
    obs_count = uneven_parts(splits[6], N_TILE, N_TILE * OBS_CAP // 2, OBS_CAP, 2).astype(jnp.int32)
    innovation = bell_draw(splits[7], (OBS,), 1.0, 6.0, ((0, 128),), jnp.float32)
    obs_error = jnp.clip(jnp.exp(math.log(3.0) - 2.3025851 * jax.random.uniform(splits[8], (OBS,), jnp.float32) ** block_scale(splits[8], (OBS,), ((0, 128),), -0.2, 0.2)), 0.3, 3.0)
    prior_precision = jnp.clip(jnp.exp(jax.random.uniform(splits[9], (TRACERS,), jnp.float32, math.log(0.5), math.log(2.0))), 0.5, 2.0)
    return {"tracers": tracers, "courant": courant, "vertical_mix": vertical_mix, "kernel_profile": kernel_profile, "obs_cell": obs_cell, "obs_top": obs_top, "obs_count": obs_count, "innovation": innovation, "obs_error": obs_error, "prior_precision": prior_precision}


HORIZ = 0.05

def advance(padded, wind_pad, mix_pad):
    centre = padded[:, :, 1:-1]
    left = padded[:, :, :-2]
    right = padded[:, :, 2:]
    wind_here = wind_pad[:, 1:-1]
    wind_east = wind_pad[:, 2:]
    mixing = mix_pad[:, 1:-1]
    inflow = jnp.maximum(wind_here, 0.0) * left + jnp.minimum(wind_here, 0.0) * centre
    outflow = jnp.maximum(wind_east, 0.0) * centre + jnp.minimum(wind_east, 0.0) * right
    north = jnp.concatenate([centre[..., 1:], centre[..., -1:]], -1)
    south = jnp.concatenate([centre[..., :1], centre[..., :-1]], -1)
    above = jnp.concatenate([centre[:, 1:], centre[:, -1:]], 1)
    below = jnp.concatenate([centre[:, :1], centre[:, :-1]], 1)
    return centre + inflow - outflow + HORIZ * (left + right - 2.0 * centre) + HORIZ * (north + south - 2.0 * centre) + mixing * (above + below - 2.0 * centre)

def periodic(field, axis):
    width = field.shape[axis]
    return jnp.concatenate([lax.slice_in_dim(field, width - 1, width, axis=axis), field, lax.slice_in_dim(field, 0, 1, axis=axis)], axis)

def reference(tracers, courant, vertical_mix, kernel_profile, obs_cell, obs_top, obs_count, innovation, obs_error, prior_precision):
    fields = tracers
    wind_pad = periodic(courant, 1)
    mix_pad = periodic(vertical_mix, 1)
    for step in range(STEPS):
        fields = advance(periodic(fields, 2), wind_pad, mix_pad)
    cells = obs_cell.reshape(N_TILE, OBS_CAP)
    tops = obs_top.reshape(N_TILE, OBS_CAP)
    levels = jnp.arange(LEV, dtype=jnp.int32)

    def per_tile(index):
        block = lax.dynamic_slice_in_dim(fields, index * CLON, CLON, 2).reshape(TRACERS, LEV, CLON * LAT)
        values = block[:, :, cells[index]]
        weights = kernel_profile[:, None] * (levels[:, None] < tops[index][None, :]).astype(jnp.float32)
        return jnp.einsum('tlk,lk->tk', values, weights, precision=lax.Precision.HIGHEST)
    jacobian = lax.map(per_tile, jnp.arange(N_TILE, dtype=jnp.int32))
    slots = jnp.arange(OBS_CAP, dtype=jnp.int32)
    live = (slots[None, :] < obs_count[:, None]).astype(jnp.float32)
    innov = innovation.reshape(N_TILE, OBS_CAP)
    weight = live / obs_error.reshape(N_TILE, OBS_CAP)
    weighted = jacobian * weight[:, None, :]
    gram = jnp.einsum('ntk,nsk->ts', weighted, jacobian, precision=lax.Precision.HIGHEST) + jnp.diag(prior_precision)
    gradient = jnp.einsum('ntk,nk->t', weighted, innov, precision=lax.Precision.HIGHEST)
    update = jnp.linalg.solve(gram, gradient)
    fitted = jnp.einsum('t,ntk->nk', update, jacobian, precision=lax.Precision.HIGHEST)
    misfit = (live * (innov - fitted)).reshape(OBS_CAP * N_TILE)
    return (fields, update, misfit)
```

```python
import jax
import jax.numpy as jnp
from jax import lax
from jax.experimental import pallas as pl
from jax.experimental.pallas import tpu as pltpu
from jax.sharding import Mesh
from jax.sharding import PartitionSpec as P

TILE = ("tile_0", "tile_1", "tile_2", "tile_3")
HORIZ = 0.05
LEV = 47
LEVELS = 48
TR = 16
LAT = 256
OBS = 2048
ROWS = 6 * LAT
F32 = jnp.float32
EXACT = lax.Precision.HIGHEST
GROUPS = ((0, 1),)


def own(core, p):
    return p + core * (5 - 2 * p)


def triple(core, q):
    return q + core * (2 - 2 * q)


def coefficients(core, faces, mixes, cells, cm, cp, cd):
    sign = (1 - 2 * core).astype(F32)

    def wind(p):
        return faces[p + 3 + core * (6 - 2 * p)] * sign

    for j, p in enumerate(cells):
        here, there = wind(p), wind(p + 1)
        cm[j] = jnp.maximum(here, 0.0) + HORIZ
        cp[j] = HORIZ - jnp.minimum(there, 0.0)
        mixing = mixes[own(core, p) + 2]
        cd[j] = (1.0 - 4.0 * HORIZ) + jnp.minimum(here, 0.0) - jnp.maximum(there, 0.0) - 2.0 * mixing


def across(halves, start, end):
    low, high = halves
    ahead, back = [pltpu.roll(x, 127, 1) for x in halves], [pltpu.roll(x, 1, 1) for x in halves]
    north = [jnp.where(end, ahead[1], ahead[0]), jnp.where(end, high, ahead[1])]
    south = [jnp.where(start, low, back[0]), jnp.where(start, back[0], back[1])]
    return [HORIZ * (n + s) for n, s in zip(north, south)]


def march(core, groups, cells, first, source, mixes, cm, cp, cd, emit, extra=(), unroll=8):
    lane = lax.broadcasted_iota(jnp.int32, (8, 128), 1)
    start, end = lane == 0, lane == 127
    pairs_of = [(p, g) for p in cells for g in groups]

    def load(l, p, g):
        ref, index = source(l, p)
        return [ref[(*index, pl.ds(8 * g, 8), pl.ds(128 * h, 128))] for h in (0, 1)]

    def one(level, state):
        below, here, sides, more = state
        up = jnp.minimum(level + 1, LEV - 1)
        above = {k: load(up, *k) for k in pairs_of}
        beyond = {k: across(above[k], start, end) for k in pairs_of}
        rows = {}
        for p in cells:
            row = pl.ds(level, 1)
            j, mix_at = p - first, own(core, p) + 2
            rows[p] = [jnp.broadcast_to(ref[k, row, :], (8, LAT)) for ref, k in ((cd, j), (cm, j), (cp, j), (mixes, mix_at))]
        for p, g in pairs_of:
            minus = here[p - 1, g] if p - 1 in cells else load(jnp.minimum(level, LEV - 1), p - 1, g)
            plus = here[p + 1, g] if p + 1 in cells else load(jnp.minimum(level, LEV - 1), p + 1, g)
            for h in (0, 1):
                d, m, q, mixing = (x[:, 128 * h : 128 * h + 128] for x in rows[p])
                new = (d * here[p, g][h] + sides[p, g][h]) + (m * minus[h] + q * plus[h])
                new = new + mixing * (above[p, g][h] + below[p, g][h])
                more = emit(level, p, g, h, new, more)
        return here, above, beyond, more

    def body(i, state):
        for u in range(unroll):
            state = one(i * unroll + u, state)
        return state

    bottom = {k: load(0, *k) for k in pairs_of}
    lax.fori_loop(0, LEVELS // unroll, body, (bottom, bottom, {k: across(bottom[k], start, end) for k in pairs_of}, extra))


def storing(target):
    def emit(level, p, g, h, new, more):
        ref, at = target(level, p)
        ref[(*at, pl.ds(8 * g, 8), pl.ds(128 * h, 128))] = new
        return more

    return emit


def transposed_rows(prefix, table, place):
    for q in range(3):
        for group in range(6):
            for h in (0, 1):
                block = prefix[pl.ds(8 * group, 8), q, :, pl.ds(128 * h, 128)].reshape(128, 128)
                table[pl.ds(place(q) + group * LAT + 128 * h, 128), :] = block.T


def final_step(core, groups, cells, first, source, mixes, cm, cp, cd, kp, slot, done, prefix):
    zero = jnp.zeros((8, 128), F32)

    def emit(level, p, g, h, new, sums):
        at = (level, slot(p), pl.ds(8 * g, 8), pl.ds(128 * h, 128))
        done[at] = new
        total = sums[p, g, h] + kp[level] * new
        prefix[at] = total
        return {**sums, (p, g, h): total}

    sums = {(p, g, h): zero for p in cells for g in groups for h in (0, 1)}
    march(core, groups, cells, first, source, mixes, cm, cp, cd, emit, sums)


def edge_kernel(side_ref, cells, out, sems):
    copies = []
    for k in range(4):
        levels = pl.ds(12 * k, min(12, LEV - 12 * k))
        copies.append(pltpu.make_async_copy(cells.at[levels, pl.ds(3 * side_ref[0], 3)], out.at[levels], sems.at[k]))
    for copy in copies:
        copy.start()
    for copy in copies:
        copy.wait()


def early_kernel(core_ref, kp, cells_hbm, halo, wind, mix, wind_mix_halo, out, carry, table, faces, mixes, tracers, cm, cp, cd, s1, s2, done, prefix, sem, sems):
    core = core_ref[0]
    loads = [pltpu.make_async_copy(cells_hbm.at[pl.ds(12 * k, min(12, LEV - 12 * k))], tracers.at[pl.ds(12 * k, min(12, LEV - 12 * k))], sems.at[k]) for k in range(4)]
    for load in loads:
        load.start()
    faces[3:9, :LEV] = wind[...]
    faces[pl.ds(9 - 9 * core, 3), :LEV] = wind_mix_halo[0:3]
    mixes[2:8, :LEV] = mix[...]
    mixes[pl.ds(8 - 8 * core, 2), :LEV] = wind_mix_halo[3:5]
    cells = range(1, 8)
    coefficients(core, faces, mixes, cells, cm, cp, cd)

    def source0(l, p):
        return (tracers, (l, own(core, p))) if p < 6 else (halo, (l, triple(core, p - 6)))

    def source1(l, p):
        return (carry, (l, p + 1)) if p < 3 else (s1, (l, p - 3))

    def source2(l, p):
        return (carry, (l, p + 2)) if p < 4 else (s2, (l, p - 4))

    for load in loads:
        load.wait()

    def keep(level, _):
        carry[level, 0] = tracers[level, own(core, 0)]
        carry[level, 1] = tracers[level, own(core, 1)]
        return 0

    lax.fori_loop(0, LEV, keep, 0)
    for g in range(TR // 8):
        march(core, (g,), range(1, 8), 1, source0, mixes, cm, cp, cd, storing(source1))
        march(core, (g,), range(2, 7), 1, source1, mixes, cm, cp, cd, storing(source2))
        final_step(core, (g,), range(3, 6), 1, source2, mixes, cm, cp, cd, kp, lambda p: triple(core, p - 3), done, prefix)
    copy = pltpu.make_async_copy(done.at[pl.ds(0, LEV)], out.at[:, pl.ds(3 - 3 * core, 3)], sem)
    copy.start()
    transposed_rows(prefix, table, lambda q: q * ROWS)
    copy.wait()


def late_kernel(core_ref, kp, rows, halo, carry, wind, mix, wind_mix_halo, early_table, mask, fields_in, out, jac, faces, mixes, cm, cp, cd, s1, s2, done, prefix, table, picked, sem, table_sem):
    core = core_ref[0]
    table_copy = pltpu.make_async_copy(early_table, table.at[pl.ds((3 - 3 * core) * ROWS, 3 * ROWS)], table_sem)
    table_copy.start()
    faces[3:9, :LEV] = wind[...]
    faces[pl.ds(9 * core, 3), :LEV] = wind_mix_halo[0:3]
    mixes[2:8, :LEV] = mix[...]
    mixes[pl.ds(8 * core, 2), :LEV] = wind_mix_halo[3:5]
    coefficients(core, faces, mixes, range(-2, 3), cm, cp, cd)

    def source0(l, p):
        return (carry, (l, p)) if p >= 0 else (halo, (l, triple(core, p + 3)))

    def source1(l, p):
        return (carry, (l, p + 1)) if p >= 1 else (s1, (l, p + 2))

    def source2(l, p):
        return (carry, (l, p + 2)) if p >= 2 else (s2, (l, p + 1))

    for groups in GROUPS:
        march(core, groups, range(-2, 1), -2, source0, mixes, cm, cp, cd, storing(source1))
        march(core, groups, range(-1, 2), -2, source1, mixes, cm, cp, cd, storing(source2))
        final_step(core, groups, range(0, 3), -2, source2, mixes, cm, cp, cd, kp, lambda p: triple(core, p), done, prefix)
    copy = pltpu.make_async_copy(done.at[pl.ds(0, LEV)], out.at[:, pl.ds(3 * core, 3)], sem)
    copy.start()
    transposed_rows(prefix, table, lambda q: pl.multiple_of((3 * core + q) * ROWS, ROWS))
    table_copy.wait()

    def pick(block, _):
        for u in range(16):
            k = block * 16 + u
            picked[pl.ds(k, 1), :] = table[pl.ds(rows[k], 1), :]
        return 0

    lax.fori_loop(0, OBS // 16, pick, 0)
    kept = jnp.where(mask[...] > 0.5, picked[...], 0.0)
    same = lax.broadcasted_iota(jnp.int32, (TR, 128), 1) % TR == lax.broadcasted_iota(jnp.int32, (TR, 128), 0)
    jac[...] = lax.dot_general(same.astype(F32), kept, (((1,), (1,)), ((), ())), precision=EXACT, preferred_element_type=F32)
    copy.wait()


def gram_kernel(trc_ref, mine, other, weight, innov, out, full, padded):
    trc = trc_ref[0]
    full[pl.ds(pl.multiple_of(trc * TR, TR), TR)] = mine[...]
    full[pl.ds(pl.multiple_of(TR - trc * TR, TR), TR)] = other[...]
    jac = full[...]
    padded[0:32] = jac
    padded[32:128] = jnp.zeros((96, OBS), F32)
    weighted = jac * weight[...]
    both = (((1,), (1,)), ((), ()))
    gram = lax.dot_general(weighted, padded[...], both, precision=EXACT, preferred_element_type=F32)
    lhs = jnp.broadcast_to(weight[...] * innov[...], (8, OBS))
    out[0:8] = sum((pltpu.roll(gram[8 * k : 8 * k + 8], 32 * k, 1) for k in range(1, 4)), gram[0:8])
    out[8:16] = lax.dot_general(lhs, padded[...], both, precision=EXACT, preferred_element_type=F32)


def solve_kernel(total, prior, full, live, innov, update, misfit):
    lane = lax.broadcasted_iota(jnp.int32, (32, 128), 1)
    row = lax.broadcasted_iota(jnp.int32, (32, 128), 0)
    packed = total[0:8]
    gram = jnp.concatenate([packed] + [pltpu.roll(packed, 128 - 32 * k, 1) for k in range(1, 4)], 0)
    diagonal = lane == row
    gram = gram + jnp.where(diagonal, jnp.broadcast_to(prior[...], (32, 128)), 0.0)
    side = jnp.sum(jnp.where(diagonal, jnp.broadcast_to(total[8:9], (32, 128)), 0.0), 1, keepdims=True)
    aug = jnp.where(lane < 32, gram, jnp.where(lane == 32, side, 0.0))
    for k in range(32):
        top = aug[k : k + 1] / aug[k : k + 1, k : k + 1]
        aug = jnp.where(row == k, top, aug - aug[:, k : k + 1] * top)
    answer = aug[:, 32:33]
    update[...] = jnp.sum(jnp.where(diagonal, answer, 0.0), 0)[:32]
    fitted = jnp.sum(full[...] * answer, 0, keepdims=True)
    fitted = jnp.concatenate([fitted[:, 128 * k : 128 * k + 128] for k in range(OBS // 128)], 0)
    misfit[...] = live[...] * (innov[...] - fitted)


def vmem(n):
    return [pl.BlockSpec(memory_space=pltpu.VMEM)] * n


def smem(n):
    return [pl.BlockSpec(memory_space=pltpu.SMEM)] * n


def anywhere(n):
    return [pl.BlockSpec(memory_space=pl.ANY)] * n


def of(*dims):
    return jax.ShapeDtypeStruct(dims, F32)


def work(*dims):
    return pltpu.VMEM(dims, F32)


def kept(*dims):
    return pltpu.VMEM(dims, F32)


def near(*arrays):
    return [pltpu.with_memory_space_constraint(x, pltpu.VMEM) for x in arrays]


def limit(mib):
    return pltpu.CompilerParams(vmem_limit_bytes=mib << 20)


def pairs(remote):
    n = 128
    low = [(i, (i + 1) % n) for i in range(1 if remote else 0, n, 2)]
    return low + [(j, i) for i, j in low]


def stages():
    yield "tile_3", [(i, i ^ 1) for i in range(2)]
    for flip in (1, 3):
        yield "tile_0", [(i, i ^ flip) for i in range(4)]
    for flip in (1, 2, 6):
        yield "tile_2", [(i, i ^ flip) for i in range(8)]
    yield "tile_1", [(i, i ^ 1) for i in range(2)]


def per_device(tracers, courant, vertical_mix, kernel_profile, obs_cell, obs_top, obs_count, innovation, obs_error, prior_precision):
    core = lax.axis_index("tile_3").astype(jnp.int32)
    trc = lax.axis_index("trc").astype(jnp.int32)
    core_at, trc_at = core.reshape(1), trc.reshape(1)
    cells = pltpu.with_memory_space_constraint(jnp.transpose(tracers, (1, 2, 0, 3)), pltpu.HBM)
    wind = jnp.transpose(courant, (1, 0, 2))
    mix = jnp.transpose(vertical_mix, (1, 0, 2))

    def edge(side):
        return pl.pallas_call(
            edge_kernel,
            out_shape=kept(LEV, 3, TR, LAT),
            in_specs=smem(1) + anywhere(1),
            out_specs=vmem(1)[0],
            scratch_shapes=[pltpu.SemaphoreType.DMA((4,))],
            compiler_params=limit(4),
            name="edge",
        )(side.reshape(1), cells)

    def rim(side):
        return jnp.concatenate([lax.dynamic_slice_in_dim(wind, 3 * side, 3, 0), lax.dynamic_slice_in_dim(mix, 4 * side, 2, 0)], 0)

    far_halo = lax.ppermute(edge(core), TILE, pairs(True))
    near_edge = edge(1 - core)
    near_halo = lax.ppermute(near_edge, TILE, pairs(False))
    near_rim = lax.ppermute(rim(1 - core), TILE, pairs(False))
    far_rim = lax.ppermute(rim(core), TILE, pairs(True))

    block = (LEV, 6, TR, LAT)
    profile = jnp.pad(kernel_profile, (0, LEVELS - LEV))
    fields, carry, early_table = pl.pallas_call(
        early_kernel,
        out_shape=(of(*block), kept(LEVELS, 6, TR, LAT), kept(3 * ROWS, 128)),
        in_specs=smem(2) + anywhere(1) + vmem(4),
        out_specs=anywhere(1) + vmem(2),
        scratch_shapes=[work(12, 48, LAT), work(10, 48, LAT), work(LEV, 6, TR, LAT), work(7, 48, LAT), work(7, 48, LAT), work(7, 48, LAT),
                        work(48, 5, TR, LAT), work(48, 3, TR, LAT), work(48, 3, TR, LAT), work(48, 3, TR, LAT), pltpu.SemaphoreType.DMA, pltpu.SemaphoreType.DMA((4,))],
        compiler_params=limit(30),
        cost_estimate=pl.CostEstimate(flops=10**9, transcendentals=0, bytes_accessed=15 * 10**6),
        name="early",
    )(core_at, profile, cells, *near(near_halo, wind, mix, near_rim))

    cell = jnp.clip(obs_cell, 0, 6 * LAT - 1)
    level = jnp.clip(obs_top, 1, LEV) - 1
    rows = (cell // LAT) * ROWS + (level // 8) * LAT + cell % LAT
    lanes = lax.broadcasted_iota(jnp.int32, (OBS, 128), 1) // TR
    mask = (lanes == (level % 8)[:, None]).astype(F32)
    slots = jnp.arange(OBS, dtype=jnp.int32)
    live = (slots < obs_count[0]).astype(F32)
    weight = (live / obs_error).reshape(1, OBS)

    fields, mine = pl.pallas_call(
        late_kernel,
        out_shape=(of(*block), kept(TR, OBS)),
        in_specs=smem(3) + vmem(5) + anywhere(1) + vmem(1) + anywhere(1),
        out_specs=anywhere(1) + vmem(1),
        scratch_shapes=[work(12, 48, LAT), work(10, 48, LAT), work(5, 48, LAT), work(5, 48, LAT), work(5, 48, LAT),
                        work(48, 3, TR, LAT), work(48, 3, TR, LAT), work(48, 3, TR, LAT), work(48, 3, TR, LAT),
                        work(6 * ROWS, 128), work(OBS, 128), pltpu.SemaphoreType.DMA, pltpu.SemaphoreType.DMA],
        input_output_aliases={10: 0},
        compiler_params=limit(34),
        cost_estimate=pl.CostEstimate(flops=10**9, transcendentals=0, bytes_accessed=15 * 10**6),
        name="late",
    )(core_at, profile, rows, *near(far_halo, carry, wind, mix, far_rim, early_table, mask), fields)

    other = lax.ppermute(mine, "trc", [(0, 1), (1, 0)])
    total, full = pl.pallas_call(
        gram_kernel,
        out_shape=(kept(16, 128), kept(2 * TR, OBS)),
        in_specs=smem(1) + vmem(4),
        out_specs=vmem(2),
        scratch_shapes=[work(128, OBS)],
        compiler_params=limit(8),
        name="gram",
    )(trc_at, *near(mine, other, weight, innovation.reshape(1, OBS)))
    for axis, swap in stages():
        total = total + lax.ppermute(total, axis, swap)

    prior = jnp.pad(prior_precision, (0, 96)).reshape(1, 128)
    update, misfit = pl.pallas_call(
        solve_kernel,
        out_shape=(of(32), of(OBS // 128, 128)),
        in_specs=vmem(5),
        out_specs=vmem(2),
        compiler_params=limit(4),
        name="solve",
    )(*near(total, prior, full, live.reshape(OBS // 128, 128), innovation.reshape(OBS // 128, 128)))
    return (jnp.transpose(fields, (2, 0, 1, 3)), update, misfit.reshape(OBS))


def solution(mesh):
    split = Mesh(
        mesh.devices.reshape(4, 2, 8, 2, mesh.shape["trc"]),
        ("tile_0", "tile_1", "tile_2", "tile_3", "trc"),
    )
    return jax.shard_map(
        per_device,
        mesh=split,
        in_specs=(P("trc", None, TILE, None), P(None, TILE, None), P(None, TILE, None), P(), P(TILE), P(TILE), P(TILE), P(TILE), P(TILE), P()),
        out_specs=(P("trc", None, TILE, None), P(), P(TILE)),
        check_vma=False,
    )
```

```python
import jax
import jax.numpy as jnp
from jax import lax
from jax.experimental import pallas as pl
from jax.experimental.pallas import tpu as pltpu
from jax.sharding import Mesh
from jax.sharding import PartitionSpec as P

TILE = ("tile_0", "tile_1", "tile_2", "tile_3")
HORIZ = 0.05
LEV = 47
LEVELS = 48
TR = 16
LAT = 256
OBS = 2048
ROWS = 6 * LAT
F32 = jnp.float32
EXACT = lax.Precision.HIGHEST
GROUPS = ((0, 1),)


def own(core, p):
    return p + core * (5 - 2 * p)


def triple(core, q):
    return q + core * (2 - 2 * q)


def coefficients(core, faces, mixes, cells, cm, cp, cd):
    sign = (1 - 2 * core).astype(F32)

    def wind(p):
        return faces[p + 3 + core * (6 - 2 * p)] * sign

    for j, p in enumerate(cells):
        here, there = wind(p), wind(p + 1)
        cm[j] = jnp.maximum(here, 0.0) + HORIZ
        cp[j] = HORIZ - jnp.minimum(there, 0.0)
        mixing = mixes[own(core, p) + 2]
        cd[j] = (1.0 - 4.0 * HORIZ) + jnp.minimum(here, 0.0) - jnp.maximum(there, 0.0) - 2.0 * mixing


def across(halves, start, end):
    low, high = halves
    ahead, back = [pltpu.roll(x, 127, 1) for x in halves], [pltpu.roll(x, 1, 1) for x in halves]
    north = [jnp.where(end, ahead[1], ahead[0]), jnp.where(end, high, ahead[1])]
    south = [jnp.where(start, low, back[0]), jnp.where(start, back[0], back[1])]
    return [HORIZ * (n + s) for n, s in zip(north, south)]


def march(core, groups, cells, first, source, mixes, cm, cp, cd, emit, extra=(), unroll=16):
    lane = lax.broadcasted_iota(jnp.int32, (8, 128), 1)
    start, end = lane == 0, lane == 127
    pairs_of = [(p, g) for p in cells for g in groups]

    def load(l, p, g):
        ref, index = source(l, p)
        return [ref[(*index, pl.ds(8 * g, 8), pl.ds(128 * h, 128))] for h in (0, 1)]

    def one(level, state):
        below, here, sides, more = state
        up = jnp.minimum(level + 1, LEV - 1)
        above = {k: load(up, *k) for k in pairs_of}
        beyond = {k: across(above[k], start, end) for k in pairs_of}
        rows = {}
        for p in cells:
            row = pl.ds(level, 1)
            j, mix_at = p - first, own(core, p) + 2
            rows[p] = [jnp.broadcast_to(ref[k, row, :], (8, LAT)) for ref, k in ((cd, j), (cm, j), (cp, j), (mixes, mix_at))]
        for p, g in pairs_of:
            minus = here[p - 1, g] if p - 1 in cells else load(jnp.minimum(level, LEV - 1), p - 1, g)
            plus = here[p + 1, g] if p + 1 in cells else load(jnp.minimum(level, LEV - 1), p + 1, g)
            for h in (0, 1):
                d, m, q, mixing = (x[:, 128 * h : 128 * h + 128] for x in rows[p])
                new = (d * here[p, g][h] + sides[p, g][h]) + (m * minus[h] + q * plus[h])
                new = new + mixing * (above[p, g][h] + below[p, g][h])
                more = emit(level, p, g, h, new, more)
        return here, above, beyond, more

    def body(i, state):
        for u in range(unroll):
            state = one(i * unroll + u, state)
        return state

    bottom = {k: load(0, *k) for k in pairs_of}
    lax.fori_loop(0, LEVELS // unroll, body, (bottom, bottom, {k: across(bottom[k], start, end) for k in pairs_of}, extra))


def storing(target):
    def emit(level, p, g, h, new, more):
        ref, at = target(level, p)
        ref[(*at, pl.ds(8 * g, 8), pl.ds(128 * h, 128))] = new
        return more

    return emit


def transposed_rows(prefix, table, place):
    for q in range(3):
        for group in range(6):
            for h in (0, 1):
                block = prefix[pl.ds(8 * group, 8), q, :, pl.ds(128 * h, 128)].reshape(128, 128)
                table[pl.ds(place(q) + group * LAT + 128 * h, 128), :] = block.T


def final_step(core, groups, cells, first, source, mixes, cm, cp, cd, kp, slot, done, prefix):
    zero = jnp.zeros((8, 128), F32)

    def emit(level, p, g, h, new, sums):
        at = (level, slot(p), pl.ds(8 * g, 8), pl.ds(128 * h, 128))
        done[at] = new
        total = sums[p, g, h] + kp[level] * new
        prefix[at] = total
        return {**sums, (p, g, h): total}

    sums = {(p, g, h): zero for p in cells for g in groups for h in (0, 1)}
    march(core, groups, cells, first, source, mixes, cm, cp, cd, emit, sums)


def edge_kernel(side_ref, cells, out, buffer, sems):
    legs = []
    for k in range(6):
        levels = pl.ds(8 * k, min(8, LEV - 8 * k))
        source = cells.at[levels, pl.ds(3 * side_ref[0], 3)]
        legs.append((pltpu.make_async_copy(source, buffer.at[levels], sems.at[0, k]), pltpu.make_async_copy(buffer.at[levels], out.at[levels], sems.at[1, k])))
    for first, _ in legs:
        first.start()
    for first, second in legs:
        first.wait()
        second.start()
    for _, second in legs:
        second.wait()


def early_kernel(core_ref, kp, cells_hbm, halo, wind, mix, wind_mix_halo, out, carry, table, faces, mixes, tracers, cm, cp, cd, s1, s2, done, prefix, sem, sems):
    core = core_ref[0]
    loads = [pltpu.make_async_copy(cells_hbm.at[pl.ds(12 * k, min(12, LEV - 12 * k))], tracers.at[pl.ds(12 * k, min(12, LEV - 12 * k))], sems.at[k]) for k in range(4)]
    for load in loads:
        load.start()
    faces[3:9, :LEV] = wind[...]
    faces[pl.ds(9 - 9 * core, 3), :LEV] = wind_mix_halo[0:3]
    mixes[2:8, :LEV] = mix[...]
    mixes[pl.ds(8 - 8 * core, 2), :LEV] = wind_mix_halo[3:5]
    cells = range(1, 8)
    coefficients(core, faces, mixes, cells, cm, cp, cd)

    def source0(l, p):
        return (tracers, (l, own(core, p))) if p < 6 else (halo, (l, triple(core, p - 6)))

    def source1(l, p):
        return (carry, (l, p + 1)) if p < 3 else (s1, (l, p - 3))

    def source2(l, p):
        return (carry, (l, p + 2)) if p < 4 else (s2, (l, p - 4))

    for load in loads:
        load.wait()

    def keep(level, _):
        carry[level, 0] = tracers[level, own(core, 0)]
        carry[level, 1] = tracers[level, own(core, 1)]
        return 0

    lax.fori_loop(0, LEV, keep, 0)
    for g in range(TR // 8):
        march(core, (g,), range(1, 8), 1, source0, mixes, cm, cp, cd, storing(source1))
        march(core, (g,), range(2, 7), 1, source1, mixes, cm, cp, cd, storing(source2))
        final_step(core, (g,), range(3, 6), 1, source2, mixes, cm, cp, cd, kp, lambda p: triple(core, p - 3), done, prefix)
    copy = pltpu.make_async_copy(done.at[pl.ds(0, LEV)], out.at[:, pl.ds(3 - 3 * core, 3)], sem)
    copy.start()
    transposed_rows(prefix, table, lambda q: q * ROWS)
    copy.wait()


def late_kernel(core_ref, count_ref, kp, rows, halo_hbm, carry, wind, mix, wind_mix_halo, early_table, mask, fields_in, out, jac, faces, mixes, cm, cp, cd, s1, s2, done, prefix, table, picked, halo, sem, table_sem, halo_sems):
    core = core_ref[0]
    loads = []
    for k in range(4):
        levels = pl.ds(12 * k, min(12, LEV - 12 * k))
        loads.append(pltpu.make_async_copy(halo_hbm.at[levels], halo.at[levels], halo_sems.at[k]))
    for load in loads:
        load.start()
    table_copy = pltpu.make_async_copy(early_table, table.at[pl.ds((3 - 3 * core) * ROWS, 3 * ROWS)], table_sem)
    table_copy.start()
    faces[3:9, :LEV] = wind[...]
    faces[pl.ds(9 * core, 3), :LEV] = wind_mix_halo[0:3]
    mixes[2:8, :LEV] = mix[...]
    mixes[pl.ds(8 * core, 2), :LEV] = wind_mix_halo[3:5]
    coefficients(core, faces, mixes, range(-2, 3), cm, cp, cd)
    for load in loads:
        load.wait()

    def source0(l, p):
        return (carry, (l, p)) if p >= 0 else (halo, (l, triple(core, p + 3)))

    def source1(l, p):
        return (carry, (l, p + 1)) if p >= 1 else (s1, (l, p + 2))

    def source2(l, p):
        return (carry, (l, p + 2)) if p >= 2 else (s2, (l, p + 1))

    for groups in GROUPS:
        march(core, groups, range(-2, 1), -2, source0, mixes, cm, cp, cd, storing(source1))
        march(core, groups, range(-1, 2), -2, source1, mixes, cm, cp, cd, storing(source2))
        final_step(core, groups, range(0, 3), -2, source2, mixes, cm, cp, cd, kp, lambda p: triple(core, p), done, prefix)
    copy = pltpu.make_async_copy(done.at[pl.ds(0, LEV)], out.at[:, pl.ds(3 * core, 3)], sem)
    copy.start()
    transposed_rows(prefix, table, lambda q: pl.multiple_of((3 * core + q) * ROWS, ROWS))
    table_copy.wait()

    def pick(block, _):
        for u in range(16):
            k = block * 16 + u
            picked[pl.ds(k, 1), :] = table[pl.ds(rows[k], 1), :]
        return 0

    live_blocks = (jnp.minimum(count_ref[0], OBS) + 15) // 16
    lax.fori_loop(0, live_blocks, pick, 0)
    kept = jnp.where(mask[...] > 0.5, picked[...], 0.0)
    same = lax.broadcasted_iota(jnp.int32, (TR, 128), 1) % TR == lax.broadcasted_iota(jnp.int32, (TR, 128), 0)
    jac[...] = lax.dot_general(same.astype(F32), kept, (((1,), (1,)), ((), ())), precision=EXACT, preferred_element_type=F32)
    copy.wait()


def gram_kernel(trc_ref, mine, other, weight, innov, out, full, padded):
    trc = trc_ref[0]
    full[pl.ds(pl.multiple_of(trc * TR, TR), TR)] = mine[...]
    full[pl.ds(pl.multiple_of(TR - trc * TR, TR), TR)] = other[...]
    jac = full[...]
    padded[0:32] = jac
    padded[32:128] = jnp.zeros((96, OBS), F32)
    weighted = jac * weight[...]
    both = (((1,), (1,)), ((), ()))
    gram = lax.dot_general(weighted, padded[...], both, precision=EXACT, preferred_element_type=F32)
    lhs = jnp.broadcast_to(weight[...] * innov[...], (8, OBS))
    out[0:8] = sum((pltpu.roll(gram[8 * k : 8 * k + 8], 32 * k, 1) for k in range(1, 4)), gram[0:8])
    out[8:16] = lax.dot_general(lhs, padded[...], both, precision=EXACT, preferred_element_type=F32)


def solve_kernel(total, prior, full, live, innov, update, misfit):
    lane = lax.broadcasted_iota(jnp.int32, (32, 128), 1)
    row = lax.broadcasted_iota(jnp.int32, (32, 128), 0)
    packed = total[0:8]
    gram = jnp.concatenate([packed] + [pltpu.roll(packed, 128 - 32 * k, 1) for k in range(1, 4)], 0)
    diagonal = lane == row
    gram = gram + jnp.where(diagonal, jnp.broadcast_to(prior[...], (32, 128)), 0.0)
    side = jnp.sum(jnp.where(diagonal, jnp.broadcast_to(total[8:9], (32, 128)), 0.0), 1, keepdims=True)
    aug = jnp.where(lane < 32, gram, jnp.where(lane == 32, side, 0.0))
    for k in range(0, 32, 2):
        one, two = aug[k : k + 1], aug[k + 1 : k + 2]
        left = jnp.broadcast_to(aug[:, k : k + 1], (32, 128))
        right = jnp.broadcast_to(aug[:, k + 1 : k + 2], (32, 128))
        p, q = left[k : k + 1], right[k : k + 1]
        r, t = left[k + 1 : k + 2], right[k + 1 : k + 2]
        inverse = 1.0 / p
        ratio = r * inverse
        second = (two - one * ratio) / (t - q * ratio)
        first = (one - q * second) * inverse
        aug = jnp.where(row == k, first, jnp.where(row == k + 1, second, aug - (left * first + right * second)))
    answer = aug[:, 32:33]
    update[...] = jnp.sum(jnp.where(diagonal, answer, 0.0), 0)[:32]
    fitted = jnp.sum(full[...] * answer, 0, keepdims=True)
    fitted = jnp.concatenate([fitted[:, 128 * k : 128 * k + 128] for k in range(OBS // 128)], 0)
    misfit[...] = live[...] * (innov[...] - fitted)


def vmem(n):
    return [pl.BlockSpec(memory_space=pltpu.VMEM)] * n


def smem(n):
    return [pl.BlockSpec(memory_space=pltpu.SMEM)] * n


def anywhere(n):
    return [pl.BlockSpec(memory_space=pl.ANY)] * n


def of(*dims):
    return jax.ShapeDtypeStruct(dims, F32)


def work(*dims):
    return pltpu.VMEM(dims, F32)


def kept(*dims):
    return pltpu.VMEM(dims, F32)


def near(*arrays):
    return [pltpu.with_memory_space_constraint(x, pltpu.VMEM) for x in arrays]


def limit(mib):
    return pltpu.CompilerParams(vmem_limit_bytes=mib << 20)


def pairs(remote):
    n = 128
    low = [(i, (i + 1) % n) for i in range(1 if remote else 0, n, 2)]
    return low + [(j, i) for i, j in low]


def stages():
    yield "tile_3", [(i, i ^ 1) for i in range(2)]
    for flip in (1, 3):
        yield "tile_0", [(i, i ^ flip) for i in range(4)]
    for flip in (1, 2, 6):
        yield "tile_2", [(i, i ^ flip) for i in range(8)]
    yield "tile_1", [(i, i ^ 1) for i in range(2)]


def per_device(tracers, courant, vertical_mix, kernel_profile, obs_cell, obs_top, obs_count, innovation, obs_error, prior_precision):
    core = lax.axis_index("tile_3").astype(jnp.int32)
    trc = lax.axis_index("trc").astype(jnp.int32)
    core_at, trc_at = core.reshape(1), trc.reshape(1)
    cells = pltpu.with_memory_space_constraint(jnp.transpose(tracers, (1, 2, 0, 3)), pltpu.HBM)
    wind = jnp.transpose(courant, (1, 0, 2))
    mix = jnp.transpose(vertical_mix, (1, 0, 2))

    def edge(side):
        return pl.pallas_call(
            edge_kernel,
            out_shape=of(LEV, 3, TR, LAT),
            in_specs=smem(1) + anywhere(1),
            out_specs=anywhere(1)[0],
            scratch_shapes=[work(LEV, 3, TR, LAT), pltpu.SemaphoreType.DMA((2, 6))],
            compiler_params=limit(4),
            name="edge",
        )(side.reshape(1), cells)

    def rim(side):
        return jnp.concatenate([lax.dynamic_slice_in_dim(wind, 3 * side, 3, 0), lax.dynamic_slice_in_dim(mix, 4 * side, 2, 0)], 0)

    far_halo = lax.ppermute(edge(core), TILE, pairs(True))
    near_edge = edge(1 - core)
    near_halo = lax.ppermute(near_edge, TILE, pairs(False))
    near_rim = lax.ppermute(rim(1 - core), TILE, pairs(False))
    far_rim = lax.ppermute(rim(core), TILE, pairs(True))

    block = (LEV, 6, TR, LAT)
    profile = jnp.pad(kernel_profile, (0, LEVELS - LEV))
    fields, carry, early_table = pl.pallas_call(
        early_kernel,
        out_shape=(of(*block), kept(LEVELS, 6, TR, LAT), kept(3 * ROWS, 128)),
        in_specs=smem(2) + anywhere(1) + vmem(4),
        out_specs=anywhere(1) + vmem(2),
        scratch_shapes=[work(12, 48, LAT), work(10, 48, LAT), work(LEV, 6, TR, LAT), work(7, 48, LAT), work(7, 48, LAT), work(7, 48, LAT),
                        work(48, 5, TR, LAT), work(48, 3, TR, LAT), work(48, 3, TR, LAT), work(48, 3, TR, LAT), pltpu.SemaphoreType.DMA, pltpu.SemaphoreType.DMA((4,))],
        compiler_params=limit(30),
        cost_estimate=pl.CostEstimate(flops=10**9, transcendentals=0, bytes_accessed=15 * 10**6),
        name="early",
    )(core_at, profile, cells, *near(near_halo, wind, mix, near_rim))

    cell = jnp.clip(obs_cell, 0, 6 * LAT - 1)
    level = jnp.clip(obs_top, 1, LEV) - 1
    rows = (cell // LAT) * ROWS + (level // 8) * LAT + cell % LAT
    lanes = lax.broadcasted_iota(jnp.int32, (OBS, 128), 1) // TR
    slots = jnp.arange(OBS, dtype=jnp.int32)
    alive = slots < obs_count[0]
    mask = (lanes == jnp.where(alive, level % 8, -1)[:, None]).astype(F32)
    live = alive.astype(F32)
    weight = (live / obs_error).reshape(1, OBS)

    fields, mine = pl.pallas_call(
        late_kernel,
        out_shape=(of(*block), kept(TR, OBS)),
        in_specs=smem(4) + anywhere(1) + vmem(4) + anywhere(1) + vmem(1) + anywhere(1),
        out_specs=anywhere(1) + vmem(1),
        scratch_shapes=[work(12, 48, LAT), work(10, 48, LAT), work(5, 48, LAT), work(5, 48, LAT), work(5, 48, LAT),
                        work(48, 3, TR, LAT), work(48, 3, TR, LAT), work(48, 3, TR, LAT), work(48, 3, TR, LAT),
                        work(6 * ROWS, 128), work(OBS, 128), work(LEV, 3, TR, LAT), pltpu.SemaphoreType.DMA, pltpu.SemaphoreType.DMA, pltpu.SemaphoreType.DMA((4,))],
        input_output_aliases={11: 0},
        compiler_params=limit(34),
        cost_estimate=pl.CostEstimate(flops=10**9, transcendentals=0, bytes_accessed=15 * 10**6),
        name="late",
    )(core_at, obs_count, profile, rows, far_halo, *near(carry, wind, mix, far_rim, early_table, mask), fields)

    other = lax.ppermute(mine, "trc", [(0, 1), (1, 0)])
    total, full = pl.pallas_call(
        gram_kernel,
        out_shape=(kept(16, 128), kept(2 * TR, OBS)),
        in_specs=smem(1) + vmem(4),
        out_specs=vmem(2),
        scratch_shapes=[work(128, OBS)],
        compiler_params=limit(8),
        name="gram",
    )(trc_at, *near(mine, other, weight, innovation.reshape(1, OBS)))
    for axis, swap in stages():
        total = total + lax.ppermute(total, axis, swap)

    prior = jnp.pad(prior_precision, (0, 96)).reshape(1, 128)
    update, misfit = pl.pallas_call(
        solve_kernel,
        out_shape=(of(32), of(OBS // 128, 128)),
        in_specs=vmem(5),
        out_specs=vmem(2),
        compiler_params=limit(4),
        name="solve",
    )(*near(total, prior, full, live.reshape(OBS // 128, 128), innovation.reshape(OBS // 128, 128)))
    return (jnp.transpose(fields, (2, 0, 1, 3)), update, misfit.reshape(OBS))


def solution(mesh):
    split = Mesh(
        mesh.devices.reshape(4, 2, 8, 2, mesh.shape["trc"]),
        ("tile_0", "tile_1", "tile_2", "tile_3", "trc"),
    )
    return jax.shard_map(
        per_device,
        mesh=split,
        in_specs=(P("trc", None, TILE, None), P(None, TILE, None), P(None, TILE, None), P(), P(TILE), P(TILE), P(TILE), P(TILE), P(TILE), P()),
        out_specs=(P("trc", None, TILE, None), P(), P(TILE)),
        check_vma=False,
    )
```
